32 devices in a mesh: row: 4 (over z), col: 8 (over y, x, core).
Axes of the slice: x: 2, y: 2, z: 4, core: 2. Of those that a mesh axis runs over, the one named last changes fastest.
Arguments:
- pair: bfloat16 [256, 256, 128], P('row', 'col'), may hold values from -6 to 6
- mask: int32 [256], replicated, may hold values from 0 to 1, as said below
- chain: int32 [256], replicated, may hold values from 0 to 3, never falling along the last dimension, each value on 1 to 128 neighbouring positions
- w_ap: bfloat16 [128, 128], replicated, may hold values from -0.5 to 0.5
- w_ag: bfloat16 [128, 128], replicated, may hold values from -0.5 to 0.5
- w_bp: bfloat16 [128, 128], replicated, may hold values from -0.5 to 0.5
- w_bg: bfloat16 [128, 128], replicated, may hold values from -0.5 to 0.5
- w_gate: bfloat16 [128, 128], replicated, may hold values from -0.5 to 0.5
- w_out: bfloat16 [128, 128], replicated, may hold values from -0.5 to 0.5
- chain_bias: float32 [128], replicated, may hold values from -4 to 4
Outputs:
- update: bfloat16 [256, 256, 128], P('row', 'col')
The draws below stay inside these ranges and needn't reach their ends.
Inputs may be any that keep to these rules, and one draw needn't show every extreme that they name: `mask`: tokens from some position between 128 and 256 on are all padding (0); before it about one token in sixteen is 0 too.
All inputs are finite; a program needn't handle non-finite values.
Results may differ from the reference program's by a relative error of at most 0.012.
Values may be sent and summed in bfloat16 or wider, within the bound.
A program may use at most 64 MiB of HBM per device.

```python
import math
import jax
import jax.numpy as jnp
import numpy as np
from jax import lax

C = 128
CH = 128
N = 256


def draw_mask(key, part):
    first = jax.random.fold_in(key, 11)
    second = jax.random.fold_in(key, 12)
    length = jax.random.randint(first, (), N // 2, N + 1)
    position = jnp.arange(N)
    holes = jax.random.randint(second, (N,), 0, 16) != 0
    return ((position < length) & holes).astype(jnp.int32)


def shard_levels(key, extent, shards, low, high):
    def one(dim, parts):
        steps = jax.random.uniform(jax.random.fold_in(jax.random.fold_in(key, 6), dim), (parts,), jnp.float32, low / len(shards), high / len(shards))
        return jnp.repeat(jnp.exp(steps), extent[dim] // parts).reshape((-1,) + (1,) * (len(extent) - dim - 1))

    level = one(*shards[0])
    for cut in shards[1:]:
        level = level * one(*cut)
    return level


def length_profile(count, total, most, slope):
    loads = [(1 << 20) // math.isqrt(rank ** slope) + 1 for rank in range(2, count + 1)]
    rest, counts = total - most - (count - 1), [1] * (count - 1)
    while rest > 0:
        free = [i for i in range(count - 1) if counts[i] < most]
        mass, remaining = sum([loads[i] for i in free]), rest
        for i in free:
            addition = min(most - counts[i], max(1, remaining * loads[i] // mass), rest)
            counts[i] = counts[i] + addition
            rest = rest - addition
    return np.array([most] + counts)


def ragged(own_key, count, total, bound, slope):
    if count == 2:
        one = jax.random.randint(own_key, (), max(1, total - bound), min(bound, total - 1) + 1)
        return jnp.stack([one, total - one])
    sizes = jnp.asarray(length_profile(count, total, bound, slope), jnp.int32)
    pairs = (count - 1) // 2
    giver, receiver = sizes[1:1 + 2 * pairs:2], sizes[2:2 + 2 * pairs:2]
    slack = jnp.minimum(giver - 1, bound - receiver)
    passed = jax.random.randint(jax.random.fold_in(own_key, 1), (pairs,), 0, 1 << 20) % (slack + 1)
    sizes = sizes.at[1:1 + 2 * pairs:2].set(giver - passed).at[2:2 + 2 * pairs:2].set(receiver + passed)
    return sizes[jax.random.permutation(jax.random.fold_in(own_key, 2), count)]


def scatter_about(rng, dims, scale, bound, pieces=(), dtype=jnp.bfloat16):
    gain = shard_levels(rng, dims, pieces, -0.22, 0.18) if pieces else 1.0
    entries = jax.random.normal(rng, dims, jnp.float32) * scale * gain
    return jnp.minimum(jnp.maximum(entries, -bound), bound).astype(dtype)


def setup_inputs(seed: int = 0) -> dict:
    seeds = jax.random.split(jax.random.key(seed), 11)
    pair = scatter_about(seeds[0], (N, N, C), 1.0, 6.0, ((0, 4), (1, 8)))
    mask = draw_mask(jax.random.fold_in(seeds[10], 71), 0)
    chain = jnp.searchsorted(jnp.cumsum(ragged(seeds[2], 4, N, N // 2, 0)), jnp.arange(N), side="right").astype(jnp.int32)
    w_ap = scatter_about(seeds[3], (C, CH), C ** -0.5, 0.5)
    w_ag = scatter_about(seeds[4], (C, CH), C ** -0.5, 0.5)
    w_bp = scatter_about(seeds[5], (C, CH), C ** -0.5, 0.5)
    w_bg = scatter_about(seeds[6], (C, CH), C ** -0.5, 0.5)
    w_gate = scatter_about(seeds[7], (C, C), C ** -0.5, 0.5)
    w_out = scatter_about(seeds[8], (CH, C), CH ** -0.5, 0.5)
    chain_bias = scatter_about(seeds[9], (C,), 1.0, 4.0, (), jnp.float32)
    return {"pair": pair, "mask": mask, "chain": chain, "w_ap": w_ap, "w_ag": w_ag, "w_bp": w_bp, "w_bg": w_bg, "w_gate": w_gate, "w_out": w_out, "chain_bias": chain_bias}


def normalize(values):
    mean = lax.optimization_barrier(jnp.mean(values, axis=-1, keepdims=True))
    centred = values - mean
    spread = lax.optimization_barrier(jnp.mean(centred * centred, axis=-1, keepdims=True))
    return centred * lax.rsqrt(spread + 1e-05)

def reference(pair, mask, chain, w_ap, w_ag, w_bp, w_bg, w_gate, w_out, chain_bias):
    zn = normalize(pair.astype(jnp.float32)).astype(jnp.bfloat16)
    flat = zn.reshape(N * N, C)

    def project(weight):
        return jnp.dot(flat, weight, preferred_element_type=jnp.float32)
    mask_f = mask.astype(jnp.float32)
    pair_mask = (mask_f[:, None] * mask_f[None, :]).reshape(N * N, 1)
    left = (pair_mask * jax.nn.sigmoid(project(w_ag)) * project(w_ap)).astype(jnp.bfloat16).reshape(N, N, CH)
    right = (pair_mask * jax.nn.sigmoid(project(w_bg)) * project(w_bp)).astype(jnp.bfloat16).reshape(N, N, CH)
    mixed = jnp.einsum('kic,kjc->ijc', left.astype(jnp.float32), right.astype(jnp.float32))
    normed = normalize(mixed).astype(jnp.bfloat16).reshape(N * N, CH)
    output = jnp.dot(normed, w_out, preferred_element_type=jnp.float32)
    same = (chain[:, None] == chain[None, :]).astype(jnp.float32).reshape(N * N, 1)
    gate = project(w_gate) + same * chain_bias[None, :]
    update = (jax.nn.sigmoid(gate) * output).astype(jnp.bfloat16)
    return update.reshape(N, N, C)
```

```python
import jax
import jax.numpy as jnp
from jax import lax
from jax.sharding import PartitionSpec as P


def channel_norm(values, axis):
    mean = jnp.mean(values, axis=axis, keepdims=True)
    centred = values - mean
    spread = jnp.mean(centred * centred, axis=axis, keepdims=True)
    return centred * lax.rsqrt(spread + 1e-05)


def shards(pair, mask, chain, w_ap, w_ag, w_bp, w_bg, w_gate, w_out, chain_bias):
    tok_i, tok_j, width = pair.shape
    hidden = w_ap.shape[1]
    row_index = lax.axis_index("row")
    col_index = lax.axis_index("col")
    row_start = row_index * tok_i
    col_start = col_index * tok_j
    mask_f = mask.astype(jnp.float32)
    mask_rows = lax.dynamic_slice_in_dim(mask_f, row_start, tok_i, 0)
    mask_cols = lax.dynamic_slice_in_dim(mask_f, col_start, tok_j, 0)
    zn = channel_norm(pair.astype(jnp.float32), -1).astype(jnp.bfloat16)
    flat = zn.reshape(tok_i * tok_j, width)
    stacked = jnp.concatenate([w_ap, w_ag, w_bp, w_bg], axis=1)
    projected = jnp.dot(flat, stacked, preferred_element_type=jnp.float32)
    pair_mask = (mask_rows[:, None] * mask_cols[None, :]).reshape(tok_i * tok_j, 1)
    left_p = projected[:, 0:hidden]
    left_g = projected[:, hidden : 2 * hidden]
    right_p = projected[:, 2 * hidden : 3 * hidden]
    right_g = projected[:, 3 * hidden : 4 * hidden]
    left_own = (pair_mask * jax.nn.sigmoid(left_g) * left_p).astype(jnp.bfloat16)
    right_own = (pair_mask * jax.nn.sigmoid(right_g) * right_p).astype(jnp.bfloat16)
    axes = ("row", "col")
    n_row, n_col = lax.axis_size("row"), lax.axis_size("col")
    n_dev = n_row * n_col
    own = hidden // n_dev
    both = jnp.stack([left_own, right_own]).reshape(2, tok_i * tok_j, n_dev, own)
    both = both.transpose(2, 0, 3, 1)
    both = lax.all_to_all(both, axes, split_axis=0, concat_axis=0, tiled=True)
    both = both.reshape(n_row, n_col, 2, own, tok_i, tok_j).transpose(2, 3, 0, 4, 1, 5)
    both = both.reshape(2, own, n_row * tok_i, n_col * tok_j)
    product = jnp.einsum("cki,ckj->cij", both[0], both[1], preferred_element_type=jnp.float32)
    product = product.astype(jnp.bfloat16).reshape(own, n_row, tok_i, n_col, tok_j)
    product = product.transpose(1, 3, 0, 2, 4).reshape(n_dev, own, tok_i * tok_j)
    mixed = lax.all_to_all(product, axes, split_axis=0, concat_axis=0, tiled=True)
    mixed = mixed.reshape(hidden, tok_i * tok_j).astype(jnp.float32)
    normed = channel_norm(mixed, 0).astype(jnp.bfloat16)
    output = jnp.einsum("cp,cd->pd", normed, w_out, preferred_element_type=jnp.float32)
    chain_rows = lax.dynamic_slice_in_dim(chain, row_start, tok_i, 0)
    chain_cols = lax.dynamic_slice_in_dim(chain, col_start, tok_j, 0)
    same = (
        (chain_rows[:, None] == chain_cols[None, :]).astype(jnp.float32).reshape(tok_i * tok_j, 1)
    )
    gate = jnp.dot(flat, w_gate, preferred_element_type=jnp.float32) + same * chain_bias[None, :]
    update = (jax.nn.sigmoid(gate) * output).astype(jnp.bfloat16)
    return update.reshape(tok_i, tok_j, width)


def solution(mesh):
    return jax.shard_map(
        shards,
        mesh=mesh,
        in_specs=(P("row", "col", None), P(), P(), P(), P(), P(), P(), P(), P(), P()),
        out_specs=P("row", "col", None),
        check_vma=False,
    )
```

```python
import functools

import jax
import jax.numpy as jnp
from jax import lax
from jax.experimental import pallas as pl
from jax.experimental.pallas import tpu as pltpu
from jax.sharding import PartitionSpec as P

MESH = pl.DeviceIdType.MESH
F32 = jnp.float32
BF16 = jnp.bfloat16
LANES = 128


def swap_lane_groups(parts):
    count = len(parts)
    width = LANES // count
    parts = list(parts)
    group = lax.broadcasted_iota(jnp.int32, parts[0].shape, 1) // width
    step = 1
    while step < count:
        high = (group // step) % 2 == 1
        moved = list(parts)
        for g in range(count):
            if (g // step) % 2 == 0:
                low_part, high_part = parts[g], parts[g + step]
                moved[g] = jnp.where(high, pltpu.roll(high_part, step * width, 1), low_part)
                moved[g + step] = jnp.where(
                    high, high_part, pltpu.roll(low_part, LANES - step * width, 1)
                )
        parts = moved
        step *= 2
    return parts


def kernel(
    n_row,
    n_col,
    pair_ref,
    mask_ref,
    chain_ref,
    w_ap_ref,
    w_ag_ref,
    w_bp_ref,
    w_bg_ref,
    w_gate_ref,
    w_out_ref,
    bias_ref,
    out_ref,
    zn_ref,
    wt_ref,
    gate_ref,
    left_ref,
    right_ref,
    send_ref,
    recv_ref,
    a_ref,
    b_ref,
    x_ref,
    xsend_ref,
    xrecv_ref,
    mixed_ref,
    send_sem,
    recv_sem,
    xsend_sem,
    xrecv_sem,
):
    n_dev = n_row * n_col
    tok_i, tok_j, width = pair_ref.shape
    hidden = w_ap_ref.shape[1]
    own = hidden // n_dev
    groups = LANES // tok_j
    high = tok_i // groups
    tokens = mask_ref.shape[1]
    halves = n_col // groups
    row = lax.axis_index("row")
    col = lax.axis_index("col")
    me = row * n_col + col

    def peer(offset):
        other = lax.rem(me + offset, n_dev)
        return other, (lax.div(other, n_col), lax.rem(other, n_col))

    barrier = pltpu.get_barrier_semaphore()

    @pl.loop(1, n_dev)
    def _(offset):
        pl.semaphore_signal(barrier, inc=1, device_id=peer(offset)[1], device_id_type=MESH)

    def transposed(ref):
        return jnp.transpose(ref[...].astype(F32))

    mats = [transposed(ref).astype(BF16) for ref in (w_ap_ref, w_ag_ref, w_bp_ref, w_bg_ref)]
    for c in range(own):
        for m in range(4):
            wt_ref[c, m * n_dev : (m + 1) * n_dev, :] = mats[m][c * n_dev : (c + 1) * n_dev]

    lane = lax.broadcasted_iota(jnp.int32, (tokens, LANES), 1)
    token = lax.broadcasted_iota(jnp.int32, (tokens, LANES), 0)
    pick = jnp.where(token == col * tok_j + lane % tok_j, 1.0, 0.0).astype(BF16)
    token_row = lax.broadcasted_iota(jnp.int32, (high, tokens), 1)
    high_row = lax.broadcasted_iota(jnp.int32, (high, tokens), 0)
    group = lax.broadcasted_iota(jnp.int32, (high, LANES), 1) // tok_j

    def spread(ref):
        values = ref[...].astype(F32)
        wide = jnp.broadcast_to(values, (high, tokens))
        cols = jnp.dot(wide.astype(BF16), pick, preferred_element_type=F32)
        rows = jnp.zeros((high, LANES), F32)
        for g in range(groups):
            hit = token_row == row * tok_i + g * high + high_row
            value = jnp.sum(jnp.where(hit, wide, 0.0), axis=1, keepdims=True)
            rows = jnp.where(group == g, value, rows)
        return rows, cols

    mask_rows, mask_cols = spread(mask_ref)
    pair_mask = mask_rows * mask_cols
    chain_rows, chain_cols = spread(chain_ref)
    same = jnp.where(chain_rows == chain_cols, 1.0, 0.0)

    @pl.loop(0, high)
    def _(h):
        block = jnp.concatenate([pair_ref[g * high + h] for g in range(groups)], axis=0)
        z = jnp.transpose(block.astype(F32))
        z = z - jnp.mean(z, axis=0, keepdims=True)
        spread_z = jnp.mean(z * z, axis=0, keepdims=True)
        zn_ref[h] = (z * lax.rsqrt(spread_z + 1e-05)).astype(BF16)

    pl.semaphore_wait(barrier, n_dev - 1)

    for c in range(own):
        for h in range(high):
            y = jnp.dot(wt_ref[c], zn_ref[h], preferred_element_type=F32)
            m = pair_mask[h : h + 1, :]
            left = m * jax.nn.sigmoid(y[n_dev : 2 * n_dev]) * y[:n_dev]
            right = m * jax.nn.sigmoid(y[3 * n_dev :]) * y[2 * n_dev : 3 * n_dev]
            left_ref[pl.ds(h, n_dev, stride=high), :] = left
            right_ref[pl.ds(h, n_dev, stride=high), :] = right
        send_ref[c, :, 0] = left_ref[...].astype(BF16).reshape(n_dev, high, LANES)
        send_ref[c, :, 1] = right_ref[...].astype(BF16).reshape(n_dev, high, LANES)
        recv_ref[c, me] = send_ref[c, me]

        @pl.loop(1, n_dev)
        def _(offset):
            other, place = peer(offset)
            pltpu.make_async_remote_copy(
                src_ref=send_ref.at[c, other],
                dst_ref=recv_ref.at[c, me],
                send_sem=send_sem.at[c],
                recv_sem=recv_sem.at[c],
                device_id=place,
                device_id_type=MESH,
            ).start()

    def wait_all(ref, sem):
        part = ref.at[pl.ds(0, n_dev - 1)]
        pltpu.make_async_copy(part, part, sem).wait()

    w_gate = transposed(w_gate_ref).astype(BF16)
    w_out = transposed(w_out_ref).astype(BF16)
    bias = jnp.transpose(jnp.broadcast_to(bias_ref[...], (LANES, width)))
    for h in range(high):
        gate = jnp.dot(w_gate, zn_ref[h], preferred_element_type=F32) + same[h : h + 1, :] * bias
        gate_ref[h] = jax.nn.sigmoid(gate)

    for c in range(own):
        wait_all(recv_ref.at[c], recv_sem.at[c])
        for which, target in ((0, a_ref), (1, b_ref)):
            for r in range(n_row):
                for q in range(halves):
                    base = r * n_col + q * groups
                    parts = [recv_ref[c, base + g, which].astype(F32) for g in range(groups)]
                    for g, part in enumerate(swap_lane_groups(parts)):
                        start = r * tok_i + g * high
                        target[start : start + high, q * LANES : (q + 1) * LANES] = part.astype(
                            BF16
                        )
        x_ref[...] = lax.dot_general(
            a_ref[...], b_ref[...], (((0,), (0,)), ((), ())), preferred_element_type=F32
        )
        for r in range(n_row):
            for q in range(halves):
                parts = [
                    x_ref[
                        r * tok_i + g * high : r * tok_i + (g + 1) * high,
                        q * LANES : (q + 1) * LANES,
                    ]
                    for g in range(groups)
                ]
                for g, part in enumerate(swap_lane_groups(parts)):
                    xsend_ref[c, r * n_col + q * groups + g] = part.astype(BF16)
        xrecv_ref[c, me] = xsend_ref[c, me]

        @pl.loop(1, n_dev)
        def _(offset):
            other, place = peer(offset)
            pltpu.make_async_remote_copy(
                src_ref=xsend_ref.at[c, other],
                dst_ref=xrecv_ref.at[c, me],
                send_sem=xsend_sem.at[c],
                recv_sem=xrecv_sem.at[c],
                device_id=place,
                device_id_type=MESH,
            ).start()

    for c in range(own):
        wait_all(xrecv_ref.at[c], xrecv_sem.at[c])
        span = n_dev * high
        mixed_ref[c * span : (c + 1) * span, :] = (
            xrecv_ref[c].astype(F32).reshape(span, LANES)
        )

    for h in range(high):
        x = mixed_ref[pl.ds(h, hidden, stride=high), :]
        x = x - jnp.mean(x, axis=0, keepdims=True)
        spread_x = jnp.mean(x * x, axis=0, keepdims=True)
        xn = (x * lax.rsqrt(spread_x + 1e-05)).astype(BF16)
        value = jnp.dot(w_out, xn, preferred_element_type=F32) * gate_ref[h]
        value = jnp.transpose(value).astype(BF16)
        for g in range(groups):
            out_ref[g * high + h] = value[g * tok_j : (g + 1) * tok_j, :]

    for c in range(own):
        wait_all(send_ref.at[c], send_sem.at[c])
        wait_all(xsend_ref.at[c], xsend_sem.at[c])


def shards(n_row, n_col, pair, mask, chain, w_ap, w_ag, w_bp, w_bg, w_gate, w_out, chain_bias):
    tok_i, tok_j, width = pair.shape
    hidden = w_ap.shape[1]
    n_dev = n_row * n_col
    own = hidden // n_dev
    groups = LANES // tok_j
    high = tok_i // groups
    tokens = mask.shape[0]
    vmem = pl.BlockSpec(memory_space=pltpu.VMEM)
    return pl.pallas_call(
        functools.partial(kernel, n_row, n_col),
        out_shape=jax.ShapeDtypeStruct(pair.shape, BF16),
        in_specs=[vmem] * 10,
        out_specs=vmem,
        scratch_shapes=[
            pltpu.VMEM((high, width, LANES), BF16),
            pltpu.VMEM((own, 4 * n_dev, width), BF16),
            pltpu.VMEM((high, width, LANES), F32),
            pltpu.VMEM((n_dev * high, LANES), F32),
            pltpu.VMEM((n_dev * high, LANES), F32),
            pltpu.VMEM((own, n_dev, 2, high, LANES), BF16),
            pltpu.VMEM((own, n_dev, 2, high, LANES), BF16),
            pltpu.VMEM((tokens, tokens), BF16),
            pltpu.VMEM((tokens, tokens), BF16),
            pltpu.VMEM((tokens, tokens), F32),
            pltpu.VMEM((own, n_dev, high, LANES), BF16),
            pltpu.VMEM((own, n_dev, high, LANES), BF16),
            pltpu.VMEM((hidden * high, LANES), F32),
            pltpu.SemaphoreType.DMA((own,)),
            pltpu.SemaphoreType.DMA((own,)),
            pltpu.SemaphoreType.DMA((own,)),
            pltpu.SemaphoreType.DMA((own,)),
        ],
        compiler_params=pltpu.CompilerParams(collective_id=0, has_side_effects=True),
        name="triangle",
    )(
        pair,
        mask.reshape(1, tokens),
        chain.reshape(1, tokens),
        w_ap,
        w_ag,
        w_bp,
        w_bg,
        w_gate,
        w_out,
        chain_bias.reshape(1, width),
    )


def solution(mesh):
    return jax.shard_map(
        functools.partial(shards, mesh.shape["row"], mesh.shape["col"]),
        mesh=mesh,
        in_specs=(P("row", "col", None), P(), P(), P(), P(), P(), P(), P(), P(), P()),
        out_specs=P("row", "col", None),
        check_vma=False,
    )
```

```python
import functools

import jax
import jax.numpy as jnp
from jax import lax
from jax.experimental import pallas as pl
from jax.experimental.pallas import tpu as pltpu
from jax.sharding import PartitionSpec as P

MESH = pl.DeviceIdType.MESH
F32 = jnp.float32
BF16 = jnp.bfloat16
LANES = 128


def swap_lane_groups(parts):
    count = len(parts)
    width = LANES // count
    parts = list(parts)
    group = lax.broadcasted_iota(jnp.int32, parts[0].shape, 1) // width
    step = 1
    while step < count:
        high = (group // step) % 2 == 1
        moved = list(parts)
        for g in range(count):
            if (g // step) % 2 == 0:
                low_part, high_part = parts[g], parts[g + step]
                moved[g] = jnp.where(high, pltpu.roll(high_part, step * width, 1), low_part)
                moved[g + step] = jnp.where(
                    high, high_part, pltpu.roll(low_part, LANES - step * width, 1)
                )
        parts = moved
        step *= 2
    return parts


def kernel(
    n_row,
    n_col,
    pair_ref,
    mask_ref,
    chain_ref,
    w_ap_ref,
    w_ag_ref,
    w_bp_ref,
    w_bg_ref,
    w_gate_ref,
    w_out_ref,
    bias_ref,
    out_ref,
    zn_ref,
    wt_ref,
    gate_ref,
    left_ref,
    right_ref,
    send_ref,
    recv_ref,
    a_ref,
    b_ref,
    x_ref,
    keep_ref,
    psend_ref,
    precv_ref,
    xsend_ref,
    xrecv_ref,
    mixed_ref,
    send_sem,
    recv_sem,
    psend_sem,
    precv_sem,
    xsend_sem,
    xrecv_sem,
):
    half = n_row // 2
    n_dev = half * n_col
    tok_i, tok_j, width = pair_ref.shape
    hidden = w_ap_ref.shape[1]
    own = hidden // n_dev
    groups = LANES // tok_j
    high = tok_i // groups
    tokens = mask_ref.shape[1]
    halves = n_col // groups
    row = lax.axis_index("row")
    col = lax.axis_index("col")
    base = lax.div(row, half) * half
    far = n_row - half - base
    me = (row - base) * n_col + col
    partner = (lax.rem(row + half, n_row), col)

    def peer(offset):
        other = lax.rem(me + offset, n_dev)
        return other, (base + lax.div(other, n_col), lax.rem(other, n_col))

    barrier = pltpu.get_barrier_semaphore()

    @pl.loop(1, n_dev)
    def _(offset):
        pl.semaphore_signal(barrier, inc=1, device_id=peer(offset)[1], device_id_type=MESH)

    pl.semaphore_signal(barrier, inc=1, device_id=partner, device_id_type=MESH)

    def transposed(ref):
        return jnp.transpose(ref[...].astype(F32))

    mats = [transposed(ref).astype(BF16) for ref in (w_ap_ref, w_ag_ref, w_bp_ref, w_bg_ref)]
    for c in range(own):
        for m in range(4):
            wt_ref[c, m * n_dev : (m + 1) * n_dev, :] = mats[m][c * n_dev : (c + 1) * n_dev]

    lane = lax.broadcasted_iota(jnp.int32, (tokens, LANES), 1)
    token = lax.broadcasted_iota(jnp.int32, (tokens, LANES), 0)
    pick = jnp.where(token == col * tok_j + lane % tok_j, 1.0, 0.0).astype(BF16)
    token_row = lax.broadcasted_iota(jnp.int32, (high, tokens), 1)
    high_row = lax.broadcasted_iota(jnp.int32, (high, tokens), 0)
    group = lax.broadcasted_iota(jnp.int32, (high, LANES), 1) // tok_j

    def spread(ref):
        values = ref[...].astype(F32)
        wide = jnp.broadcast_to(values, (high, tokens))
        cols = jnp.dot(wide.astype(BF16), pick, preferred_element_type=F32)
        rows = jnp.zeros((high, LANES), F32)
        for g in range(groups):
            hit = token_row == row * tok_i + g * high + high_row
            value = jnp.sum(jnp.where(hit, wide, 0.0), axis=1, keepdims=True)
            rows = jnp.where(group == g, value, rows)
        return rows, cols

    mask_rows, mask_cols = spread(mask_ref)
    pair_mask = mask_rows * mask_cols
    chain_rows, chain_cols = spread(chain_ref)
    same = jnp.where(chain_rows == chain_cols, 1.0, 0.0)

    @pl.loop(0, high)
    def _(h):
        block = jnp.concatenate([pair_ref[g * high + h] for g in range(groups)], axis=0)
        z = jnp.transpose(block.astype(F32))
        z = z - jnp.mean(z, axis=0, keepdims=True)
        spread_z = jnp.mean(z * z, axis=0, keepdims=True)
        zn_ref[h] = (z * lax.rsqrt(spread_z + 1e-05)).astype(BF16)

    pl.semaphore_wait(barrier, n_dev)

    for c in range(own):
        for h in range(high):
            y = jnp.dot(wt_ref[c], zn_ref[h], preferred_element_type=F32)
            m = pair_mask[h : h + 1, :]
            left = m * jax.nn.sigmoid(y[n_dev : 2 * n_dev]) * y[:n_dev]
            right = m * jax.nn.sigmoid(y[3 * n_dev :]) * y[2 * n_dev : 3 * n_dev]
            left_ref[pl.ds(h, n_dev, stride=high), :] = left
            right_ref[pl.ds(h, n_dev, stride=high), :] = right
        send_ref[c, :, 0] = left_ref[...].astype(BF16).reshape(n_dev, high, LANES)
        send_ref[c, :, 1] = right_ref[...].astype(BF16).reshape(n_dev, high, LANES)
        recv_ref[c, me] = send_ref[c, me]

        @pl.loop(1, n_dev)
        def _(offset):
            other, place = peer(offset)
            pltpu.make_async_remote_copy(
                src_ref=send_ref.at[c, other],
                dst_ref=recv_ref.at[c, me],
                send_sem=send_sem.at[c],
                recv_sem=recv_sem.at[c],
                device_id=place,
                device_id_type=MESH,
            ).start()

    def wait_all(ref, sem):
        part = ref.at[pl.ds(0, n_dev - 1)]
        pltpu.make_async_copy(part, part, sem).wait()

    w_gate = transposed(w_gate_ref).astype(BF16)
    w_out = transposed(w_out_ref).astype(BF16)
    bias = jnp.transpose(jnp.broadcast_to(bias_ref[...], (LANES, width)))
    for h in range(high):
        gate = jnp.dot(w_gate, zn_ref[h], preferred_element_type=F32) + same[h : h + 1, :] * bias
        gate_ref[h] = jax.nn.sigmoid(gate)

    def partial_copy(c):
        return pltpu.make_async_remote_copy(
            src_ref=psend_ref.at[c],
            dst_ref=precv_ref.at[c],
            send_sem=psend_sem.at[c],
            recv_sem=precv_sem.at[c],
            device_id=partner,
            device_id_type=MESH,
        )

    def token_rows(first, c, target):
        for r in range(half):
            for q in range(halves):
                parts = []
                for g in range(groups):
                    start = pl.multiple_of((first + r) * tok_i + g * high, high)
                    parts.append(x_ref[pl.ds(start, high), q * LANES : (q + 1) * LANES])
                for g, part in enumerate(swap_lane_groups(parts)):
                    target[c, r * n_col + q * groups + g] = part.astype(target.dtype)

    def multiply(c):
        wait_all(recv_ref.at[c], recv_sem.at[c])
        for which, target in ((0, a_ref), (1, b_ref)):
            for r in range(half):
                for q in range(halves):
                    first = r * n_col + q * groups
                    parts = [recv_ref[c, first + g, which].astype(F32) for g in range(groups)]
                    for g, part in enumerate(swap_lane_groups(parts)):
                        start = r * tok_i + g * high
                        target[start : start + high, q * LANES : (q + 1) * LANES] = part.astype(
                            BF16
                        )
        x_ref[...] = lax.dot_general(
            a_ref[...], b_ref[...], (((0,), (0,)), ((), ())), preferred_element_type=F32
        )
        token_rows(far, c, psend_ref)
        partial_copy(c).start()
        token_rows(base, c, keep_ref)

    def give_back(c):
        partial_copy(c).wait_recv()
        xsend_ref[c] = (keep_ref[c] + precv_ref[c].astype(F32)).astype(BF16)
        xrecv_ref[c, me] = xsend_ref[c, me]

        @pl.loop(1, n_dev)
        def _(offset):
            other, place = peer(offset)
            pltpu.make_async_remote_copy(
                src_ref=xsend_ref.at[c, other],
                dst_ref=xrecv_ref.at[c, me],
                send_sem=xsend_sem.at[c],
                recv_sem=xrecv_sem.at[c],
                device_id=place,
                device_id_type=MESH,
            ).start()

    lag = max(own // 2, 1)
    for c in range(own + lag):
        if c < own:
            multiply(c)
        if c >= lag:
            give_back(c - lag)

    for c in range(own):
        wait_all(xrecv_ref.at[c], xrecv_sem.at[c])
        span = n_dev * high
        mixed_ref[c * span : (c + 1) * span, :] = (
            xrecv_ref[c].astype(F32).reshape(span, LANES)
        )

    for h in range(high):
        x = mixed_ref[pl.ds(h, hidden, stride=high), :]
        x = x - jnp.mean(x, axis=0, keepdims=True)
        spread_x = jnp.mean(x * x, axis=0, keepdims=True)
        xn = (x * lax.rsqrt(spread_x + 1e-05)).astype(BF16)
        value = jnp.dot(w_out, xn, preferred_element_type=F32) * gate_ref[h]
        value = jnp.transpose(value).astype(BF16)
        for g in range(groups):
            out_ref[g * high + h] = value[g * tok_j : (g + 1) * tok_j, :]

    for c in range(own):
        wait_all(send_ref.at[c], send_sem.at[c])
        partial_copy(c).wait_send()
        wait_all(xsend_ref.at[c], xsend_sem.at[c])


def shards(n_row, n_col, pair, mask, chain, w_ap, w_ag, w_bp, w_bg, w_gate, w_out, chain_bias):
    tok_i, tok_j, width = pair.shape
    hidden = w_ap.shape[1]
    half = n_row // 2
    n_dev = half * n_col
    own = hidden // n_dev
    groups = LANES // tok_j
    high = tok_i // groups
    tokens = mask.shape[0]
    vmem = pl.BlockSpec(memory_space=pltpu.VMEM)
    return pl.pallas_call(
        functools.partial(kernel, n_row, n_col),
        out_shape=jax.ShapeDtypeStruct(pair.shape, BF16),
        in_specs=[vmem] * 10,
        out_specs=vmem,
        scratch_shapes=[
            pltpu.VMEM((high, width, LANES), BF16),
            pltpu.VMEM((own, 4 * n_dev, width), BF16),
            pltpu.VMEM((high, width, LANES), F32),
            pltpu.VMEM((n_dev * high, LANES), F32),
            pltpu.VMEM((n_dev * high, LANES), F32),
            pltpu.VMEM((own, n_dev, 2, high, LANES), BF16),
            pltpu.VMEM((own, n_dev, 2, high, LANES), BF16),
            pltpu.VMEM((half * tok_i, tokens), BF16),
            pltpu.VMEM((half * tok_i, tokens), BF16),
            pltpu.VMEM((tokens, tokens), F32),
            pltpu.VMEM((own, n_dev, high, LANES), F32),
            pltpu.VMEM((own, n_dev, high, LANES), BF16),
            pltpu.VMEM((own, n_dev, high, LANES), BF16),
            pltpu.VMEM((own, n_dev, high, LANES), BF16),
            pltpu.VMEM((own, n_dev, high, LANES), BF16),
            pltpu.VMEM((hidden * high, LANES), F32),
            pltpu.SemaphoreType.DMA((own,)),
            pltpu.SemaphoreType.DMA((own,)),
            pltpu.SemaphoreType.DMA((own,)),
            pltpu.SemaphoreType.DMA((own,)),
            pltpu.SemaphoreType.DMA((own,)),
            pltpu.SemaphoreType.DMA((own,)),
        ],
        compiler_params=pltpu.CompilerParams(collective_id=0, has_side_effects=True),
        name="triangle",
    )(
        pair,
        mask.reshape(1, tokens),
        chain.reshape(1, tokens),
        w_ap,
        w_ag,
        w_bp,
        w_bg,
        w_gate,
        w_out,
        chain_bias.reshape(1, width),
    )


def solution(mesh):
    return jax.shard_map(
        functools.partial(shards, mesh.shape["row"], mesh.shape["col"]),
        mesh=mesh,
        in_specs=(P("row", "col", None), P(), P(), P(), P(), P(), P(), P(), P(), P()),
        out_specs=P("row", "col", None),
        check_vma=False,
    )
```
